32 devices in a mesh: vblk: 4 (over y, x), samp: 8 (over z, core).
Axes of the slice: x: 2, y: 2, z: 4, core: 2. Of those that a mesh axis runs over, the one named last changes fastest.
Arguments:
- vectors: bfloat16 [1024, 32768], P('vblk', 'samp'), may hold values from 0 to 2, as said below
- partner: bfloat16 [1024, 32768], P('vblk', 'samp'), may hold values from 0 to 2, as said below
- next_rows: bfloat16 [1024, 32768], P(('vblk', 'samp')), may hold values from 0 to 2, as said below
Outputs:
- metric: float32 [1024, 256], P('vblk', 'samp')
- next_block: bfloat16 [1024, 32768], P('vblk', 'samp')
The draws below stay inside these ranges and needn't reach their ends.
Inputs may be any that keep to these rules, and one draw needn't show every extreme that they name: vectors: real expected allele dosages, every entry positive. partner: real expected allele dosages, every entry positive. next_rows: real expected allele dosages, every entry positive.
All inputs are finite; a program needn't handle non-finite values.
Results may differ from the reference program's by a relative error of at most 0.0004.
Values may be sent and summed in bfloat16 or wider, within the bound.
A program may use at most 64 MiB of HBM per device.

```python
import math
import jax
import jax.numpy as jnp
from jax import lax

NSAMP = 32768
NVD = 256
NVEC = 1024
NXVEC = 1024
N_VBLK = 4
N_SAMP = 8


def shard_factor(key, salt_value, low_value):
    key = jax.random.fold_in(key, salt_value)
    factors = jnp.exp(jax.random.uniform(key, (N_SAMP,), jnp.float32, math.log(low_value), 0.0))
    return jnp.repeat(factors, NSAMP // N_SAMP)[None, :]


def dosage(key, salt_value, row_count):
    common = shard_factor(key, 20, 1.0 / 30.0)
    if salt_value == 13:
        own_factor = jnp.ones((1, NSAMP), jnp.float32)
    else:
        own_factor = shard_factor(key, 20 + salt_value, 0.03)
    key = jax.random.fold_in(key, salt_value)
    subkeys = jax.random.split(key, 3)
    low = math.log(0.1)
    row_scale = jnp.exp(jax.random.uniform(subkeys[0], (row_count, 1), jnp.float32, low, 0.0))
    sample_ramp = (1.0 + 2.0 * jnp.arange(NSAMP, dtype=jnp.float32) / (NSAMP - 1)) / 3.0
    col_scale = jnp.exp(jax.random.uniform(subkeys[1], (1, NSAMP), jnp.float32, low, 0.0)) * sample_ramp[None, :]
    col_scale = col_scale * common * own_factor
    raw_values = jax.random.uniform(subkeys[2], (row_count, NSAMP), jnp.float32, 0.05, 1.0)
    return (2.0 * row_scale * col_scale * raw_values).astype(jnp.bfloat16)


def draw_vectors(key, part):
    return dosage(key, 11, NVEC)


def draw_partner(key, part):
    return dosage(key, 12, NVEC)


def draw_next_rows(key, part):
    return dosage(key, 13, NXVEC)


def setup_inputs(seed: int = 0) -> dict:
    arg_keys = jax.random.split(jax.random.key(seed), 4)
    return {
        "vectors": draw_vectors(jax.random.fold_in(arg_keys[3], 71), 0),
        "partner": draw_partner(jax.random.fold_in(arg_keys[3], 71), 0),
        "next_rows": draw_next_rows(jax.random.fold_in(arg_keys[3], 71), 0),
    }


def block_metric(own_block, pair_block):
    row_count = own_block.shape[0]
    grouped = own_block.reshape(row_count // 8, 8, own_block.shape[1])
    pair_wide = pair_block.astype(jnp.float32)

    def group_sums(row_group):
        return jnp.sum(jnp.minimum(row_group.astype(jnp.float32)[:, None, :], pair_wide[None, :, :]), axis=2)

    numerators = lax.map(group_sums, grouped).reshape(row_count, pair_block.shape[0])
    own_totals = jnp.sum(own_block.astype(jnp.float32), axis=1)
    pair_totals = jnp.sum(pair_wide, axis=1)
    return 2.0 * numerators / (own_totals[:, None] + pair_totals[None, :])


def reference(vectors, partner, next_rows):
    own_blocks = vectors.reshape(N_VBLK, NVD, NSAMP)
    pair_blocks = jnp.roll(partner.reshape(N_VBLK, NVD, NSAMP), 1, axis=0)
    metric = lax.map(lambda paired: block_metric(paired[0], paired[1]), (own_blocks, pair_blocks))
    return metric.reshape(NVEC, NVD), next_rows
```

```python
import functools

import jax
import jax.numpy as jnp
from jax import lax
from jax.experimental import pallas as pl
from jax.experimental.pallas import tpu as pltpu
from jax.sharding import PartitionSpec as P

MESH = pl.DeviceIdType.MESH
SUB = 16
LANES = 128
TREE = 8
KTILE = 256
ROWS_PER_DOT = 256
VMEM_BYTES = 60 * 1024 * 1024


def from_behind(value, axis, steps):
    count = lax.axis_size(axis)
    pairs = [(source, (source + steps) % count) for source in range(count)]
    return lax.ppermute(value, axis, pairs)


def pair_terms(row_block, col_block):
    row_count = row_block.shape[0]
    grouped = row_block.reshape(row_count // 8, 8, row_block.shape[1])

    def group_sums(row_group):
        return jnp.sum(
            jnp.minimum(row_group[:, None, :], col_block[None, :, :]), axis=2, dtype=jnp.float32
        )

    numerators = lax.map(group_sums, grouped).reshape(row_count, col_block.shape[0])
    row_totals = jnp.sum(row_block, axis=1, dtype=jnp.float32)[:, None]
    col_totals = jnp.sum(col_block, axis=1, dtype=jnp.float32)[None, :]
    return (numerators, row_totals, col_totals)


def plain_body(vectors, partner, next_rows):
    next_block = lax.all_to_all(next_rows, "samp", split_axis=1, concat_axis=0, tiled=True)
    arrived = from_behind(partner, "vblk", 1)
    numerators, row_totals, col_totals = pair_terms(vectors, arrived)
    numerators, col_totals = (
        lax.psum_scatter(numerators, "samp", scatter_dimension=1, tiled=True),
        lax.psum_scatter(col_totals, "samp", scatter_dimension=1, tiled=True),
    )
    row_totals = lax.psum(row_totals, "samp")
    metric = 2.0 * numerators / (row_totals + col_totals)
    return (metric, next_block)


def flipped(index, mask, count):
    out = 0
    bit = 1
    while bit < count:
        out = out + lax.rem(lax.div(index, bit) + lax.div(mask, bit), 2) * bit
        bit *= 2
    return out


def tree_sum(values):
    while len(values) > 1:
        values = [values[i] + values[i + 1] for i in range(0, len(values), 2)]
    return values[0]


def row_sums(block):
    ones = jnp.ones((8, block.shape[1]), jnp.bfloat16)
    return lax.dot_general(
        ones, block, (((1,), (1,)), ((), ())), preferred_element_type=jnp.float32
    )


def kernel(
    n_vblk, n_samp,
    vec_hbm, partner_hbm, next_hbm,
    total_ref, block_hbm,
    vec, wide, arrived, own_piece, part, part_in,
    vec_sem, piece_sem, pair_send, pair_recv, next_send, next_recv, part_send, part_recv,
):
    b = lax.axis_index("vblk")
    s = lax.axis_index("samp")
    up = lax.rem(b + 1, n_vblk)
    down = lax.rem(b + n_vblk - 1, n_vblk)
    row_count, samples = vec.shape
    cols = row_count // n_samp
    next_count = next_hbm.shape[0]
    group = ROWS_PER_DOT // cols
    span = samples // TREE

    vec_copy = pltpu.make_async_copy(vec_hbm, vec, vec_sem)
    vec_copy.start()
    own_in = pltpu.make_async_copy(
        next_hbm.at[:, pl.ds(pl.multiple_of(s * samples, samples), samples)],
        own_piece, piece_sem.at[0],
    )
    own_in.start()

    barrier = pltpu.get_barrier_semaphore()
    for neighbour in (up, down):
        pl.semaphore_signal(barrier, inc=1, device_id=(neighbour, s), device_id_type=MESH)
    for m in range(1, n_samp):
        pl.semaphore_signal(
            barrier, inc=1, device_id=(b, flipped(s, m, n_samp)), device_id_type=MESH
        )
    pl.semaphore_wait(barrier, n_samp + 1)

    def pair_copy(i):
        owner = flipped(s, n_samp - 1 - i, n_samp)
        return pltpu.make_async_remote_copy(
            src_ref=partner_hbm.at[pl.ds(pl.multiple_of(owner * cols, cols), cols), :],
            dst_ref=arrived.at[i],
            send_sem=pair_send.at[i], recv_sem=pair_recv.at[i],
            device_id=(up, s), device_id_type=MESH,
        )

    def next_copy(m):
        peer = flipped(s, m, n_samp)
        return pltpu.make_async_remote_copy(
            src_ref=next_hbm.at[:, pl.ds(pl.multiple_of(peer * samples, samples), samples)],
            dst_ref=block_hbm.at[pl.ds(pl.multiple_of(s * next_count, next_count), next_count), :],
            send_sem=next_send.at[m], recv_sem=next_recv.at[m],
            device_id=(b, peer), device_id_type=MESH,
        )

    def part_copy(i):
        peer = flipped(s, n_samp - 1 - i, n_samp)
        return pltpu.make_async_remote_copy(
            src_ref=part.at[i], dst_ref=part_in.at[i],
            send_sem=part_send.at[i], recv_sem=part_recv.at[i],
            device_id=(b, peer), device_id_type=MESH,
        )

    for i in range(n_samp):
        pair_copy(i).start()
    for m in range(1, n_samp):
        next_copy(m).start()

    own_in.wait()
    own_out = pltpu.make_async_copy(
        own_piece,
        block_hbm.at[pl.ds(pl.multiple_of(s * next_count, next_count), next_count), :],
        piece_sem.at[1],
    )
    own_out.start()

    vec_copy.wait()

    def widen(t, carry):
        first = pl.multiple_of(t * SUB, SUB)
        for c in range(samples // LANES):
            lanes = pl.ds(c * LANES, LANES)
            rows = vec[pl.ds(first, SUB), lanes].astype(jnp.float32)
            for r in range(SUB):
                wide[first + r, :, lanes] = jnp.broadcast_to(
                    rows[r:r + 1, :], (SUB, LANES)
                ).astype(jnp.bfloat16)
        return carry

    lax.fori_loop(0, row_count // SUB, widen, 0)

    own_totals = row_sums(vec[:, pl.ds(0, KTILE)])
    own_totals = lax.fori_loop(
        1, samples // KTILE,
        lambda k, acc: acc + row_sums(vec[:, pl.ds(pl.multiple_of(k * KTILE, KTILE), KTILE)]),
        own_totals,
    )

    groups = row_count // group

    def chunk(i, carry):
        pair_copy(i).wait_recv()

        def one_group(q):
            out = None
            for kt in range(span // KTILE):
                halves = []
                for h in range(KTILE // LANES):
                    at = [g * span + kt * KTILE + h * LANES for g in range(TREE)]
                    theirs = [
                        [arrived[i, pl.ds(j * SUB, SUB), pl.ds(o, LANES)] for o in at]
                        for j in range(cols // SUB)
                    ]
                    pieces = []
                    for r in range(group):
                        mine = [wide[q * group + r, :, pl.ds(o, LANES)] for o in at]
                        for j in range(cols // SUB):
                            pieces.append(
                                tree_sum([jnp.minimum(x, y) for x, y in zip(mine, theirs[j])])
                            )
                    halves.append(jnp.concatenate(pieces, axis=0))
                sums = row_sums(jnp.concatenate(halves, axis=1))
                out = sums if out is None else out + sums
            part[i, pl.ds(q, 1), :] = out[0:1, :]

        def groups_step(q, c):
            one_group(q)
            return c

        lax.fori_loop(0, groups, groups_step, 0)
        part[i, pl.ds(groups, 8), :] = own_totals
        part[i, pl.ds(groups + 1, 1), pl.ds(0, cols)] = row_sums(arrived[i])[0:1, :]

        @pl.when(i < n_samp - 1)
        def _():
            part_copy(i).start()

        return carry

    lax.fori_loop(0, n_samp, chunk, 0)

    total = part[n_samp - 1]
    for i in range(n_samp - 1):
        part_copy(i).wait_recv()
        total = total + part_in[i]
    total_ref[...] = total

    for i in range(n_samp):
        pair_copy(i).wait_send()
    for i in range(n_samp - 1):
        part_copy(i).wait_send()
    for m in range(1, n_samp):
        next_copy(m).wait()
    own_out.wait()


def fused_body(n_vblk, n_samp, vectors, partner, next_rows):
    rows, samples = vectors.shape
    cols = rows // n_samp
    groups = rows * cols // ROWS_PER_DOT
    part_rows = groups + 8
    next_count = next_rows.shape[0]
    hbm = pl.BlockSpec(memory_space=pl.ANY)
    dma = pltpu.SemaphoreType.DMA
    total, next_block = pl.pallas_call(
        functools.partial(kernel, n_vblk, n_samp),
        out_shape=(
            jax.ShapeDtypeStruct((part_rows, ROWS_PER_DOT), jnp.float32),
            jax.ShapeDtypeStruct((next_count * n_samp, samples), next_rows.dtype),
        ),
        in_specs=[hbm, hbm, hbm],
        out_specs=(pl.BlockSpec(memory_space=pltpu.VMEM), hbm),
        scratch_shapes=[
            pltpu.VMEM((rows, samples), jnp.bfloat16),
            pltpu.VMEM((rows, SUB, samples), jnp.bfloat16),
            pltpu.VMEM((n_samp, cols, samples), jnp.bfloat16),
            pltpu.VMEM((next_count, samples), jnp.bfloat16),
            pltpu.VMEM((n_samp, part_rows, ROWS_PER_DOT), jnp.float32),
            pltpu.VMEM((n_samp - 1, part_rows, ROWS_PER_DOT), jnp.float32),
            dma, dma((2,)),
            dma((n_samp,)), dma((n_samp,)),
            dma((n_samp,)), dma((n_samp,)),
            dma((n_samp,)), dma((n_samp,)),
        ],
        compiler_params=pltpu.CompilerParams(
            collective_id=0, has_side_effects=True, vmem_limit_bytes=VMEM_BYTES
        ),
        name="similarity",
    )(vectors, partner, next_rows)
    numerators = total[:groups].reshape(rows, cols)
    own_totals = total[groups, :rows][:, None]
    pair_totals = total[groups + 1, :cols][None, :]
    return (2.0 * numerators / (own_totals + pair_totals), next_block)


def body(n_vblk, n_samp, vectors, partner, next_rows):
    rows, samples = vectors.shape
    cols = rows // n_samp
    fits = (
        n_vblk > 2
        and n_samp > 1
        and n_samp & (n_samp - 1) == 0
        and rows == ROWS_PER_DOT
        and cols % SUB == 0
        and samples % (TREE * KTILE) == 0
        and next_rows.shape[0] % SUB == 0
        and rows * SUB * samples * 2 + 4 * rows * samples * 2 <= VMEM_BYTES
    )
    if fits:
        return fused_body(n_vblk, n_samp, vectors, partner, next_rows)
    return plain_body(vectors, partner, next_rows)


def solution(mesh):
    in_specs = (P("vblk", "samp"), P("vblk", "samp"), P(("vblk", "samp"), None))
    out_specs = (P("vblk", "samp"), P("vblk", "samp"))
    step = functools.partial(body, mesh.shape["vblk"], mesh.shape["samp"])
    return jax.shard_map(step, mesh=mesh, in_specs=in_specs, out_specs=out_specs, check_vma=False)
```

```python
import functools

import jax
import jax.numpy as jnp
from jax import lax
from jax.experimental import pallas as pl
from jax.experimental.pallas import tpu as pltpu
from jax.sharding import PartitionSpec as P

MESH = pl.DeviceIdType.MESH
SUB = 8
ALIGN = 16
WIDTH = 256
UNROLL = 2
TREE = 8
KTILE = 256
ROWS_PER_DOT = 256
VMEM_BYTES = 60 * 1024 * 1024


def from_behind(value, axis, steps):
    count = lax.axis_size(axis)
    pairs = [(source, (source + steps) % count) for source in range(count)]
    return lax.ppermute(value, axis, pairs)


def pair_terms(row_block, col_block):
    row_count = row_block.shape[0]
    grouped = row_block.reshape(row_count // 8, 8, row_block.shape[1])

    def group_sums(row_group):
        return jnp.sum(
            jnp.minimum(row_group[:, None, :], col_block[None, :, :]), axis=2, dtype=jnp.float32
        )

    numerators = lax.map(group_sums, grouped).reshape(row_count, col_block.shape[0])
    row_totals = jnp.sum(row_block, axis=1, dtype=jnp.float32)[:, None]
    col_totals = jnp.sum(col_block, axis=1, dtype=jnp.float32)[None, :]
    return (numerators, row_totals, col_totals)


def plain_body(vectors, partner, next_rows):
    next_block = lax.all_to_all(next_rows, "samp", split_axis=1, concat_axis=0, tiled=True)
    arrived = from_behind(partner, "vblk", 1)
    numerators, row_totals, col_totals = pair_terms(vectors, arrived)
    numerators, col_totals = (
        lax.psum_scatter(numerators, "samp", scatter_dimension=1, tiled=True),
        lax.psum_scatter(col_totals, "samp", scatter_dimension=1, tiled=True),
    )
    row_totals = lax.psum(row_totals, "samp")
    metric = 2.0 * numerators / (row_totals + col_totals)
    return (metric, next_block)


def flipped(index, mask, count):
    out = 0
    bit = 1
    while bit < count:
        out = out + lax.rem(lax.div(index, bit) + lax.div(mask, bit), 2) * bit
        bit *= 2
    return out


def tree_sum(values):
    while len(values) > 1:
        values = [values[i] + values[i + 1] for i in range(0, len(values), 2)]
    return values[0]


def row_sums(block):
    ones = jnp.ones((8, block.shape[1]), jnp.bfloat16)
    return lax.dot_general(
        ones, block, (((1,), (1,)), ((), ())), preferred_element_type=jnp.float32
    )


def kernel(
    n_vblk, n_samp,
    vec_hbm, partner_hbm, next_hbm,
    total_ref, block_hbm,
    vec, wide, arrived, own_piece, part, part_in,
    vec_sem, piece_sem, pair_send, pair_recv, next_send, next_recv, part_send, part_recv,
):
    b = lax.axis_index("vblk")
    s = lax.axis_index("samp")
    up = lax.rem(b + 1, n_vblk)
    down = lax.rem(b + n_vblk - 1, n_vblk)
    row_count, samples = vec.shape
    cols = row_count // n_samp
    next_count = next_hbm.shape[0]
    group = ROWS_PER_DOT // cols
    span = samples // TREE

    vec_copy = pltpu.make_async_copy(vec_hbm, vec, vec_sem)
    vec_copy.start()
    own_in = pltpu.make_async_copy(
        next_hbm.at[:, pl.ds(pl.multiple_of(s * samples, samples), samples)],
        own_piece, piece_sem.at[0],
    )
    own_in.start()

    barrier = pltpu.get_barrier_semaphore()
    for neighbour in (up, down):
        pl.semaphore_signal(barrier, inc=1, device_id=(neighbour, s), device_id_type=MESH)
    for m in range(1, n_samp):
        pl.semaphore_signal(
            barrier, inc=1, device_id=(b, flipped(s, m, n_samp)), device_id_type=MESH
        )
    pl.semaphore_wait(barrier, n_samp + 1)

    def pair_copy(i):
        owner = flipped(s, n_samp - 1 - i, n_samp)
        return pltpu.make_async_remote_copy(
            src_ref=partner_hbm.at[pl.ds(pl.multiple_of(owner * cols, cols), cols), :],
            dst_ref=arrived.at[i],
            send_sem=pair_send.at[i], recv_sem=pair_recv.at[i],
            device_id=(up, s), device_id_type=MESH,
        )

    def next_copy(m):
        peer = flipped(s, m, n_samp)
        return pltpu.make_async_remote_copy(
            src_ref=next_hbm.at[:, pl.ds(pl.multiple_of(peer * samples, samples), samples)],
            dst_ref=block_hbm.at[pl.ds(pl.multiple_of(s * next_count, next_count), next_count), :],
            send_sem=next_send.at[m], recv_sem=next_recv.at[m],
            device_id=(b, peer), device_id_type=MESH,
        )

    def part_copy(i):
        peer = flipped(s, n_samp - 1 - i, n_samp)
        return pltpu.make_async_remote_copy(
            src_ref=part.at[i], dst_ref=part_in.at[i],
            send_sem=part_send.at[i], recv_sem=part_recv.at[i],
            device_id=(b, peer), device_id_type=MESH,
        )

    for i in range(n_samp):
        pair_copy(i).start()
    for m in range(1, n_samp):
        next_copy(m).start()

    own_in.wait()
    own_out = pltpu.make_async_copy(
        own_piece,
        block_hbm.at[pl.ds(pl.multiple_of(s * next_count, next_count), next_count), :],
        piece_sem.at[1],
    )
    own_out.start()

    vec_copy.wait()

    def widen(t, carry):
        first = pl.multiple_of(t * ALIGN, ALIGN)
        for c in range(samples // WIDTH):
            lanes = pl.ds(c * WIDTH, WIDTH)
            rows = vec[pl.ds(first, ALIGN), lanes].astype(jnp.float32)
            for r in range(ALIGN):
                wide[first + r, :, lanes] = jnp.broadcast_to(
                    rows[r:r + 1, :], (SUB, WIDTH)
                ).astype(jnp.bfloat16)
        return carry

    lax.fori_loop(0, row_count // ALIGN, widen, 0)

    own_totals = row_sums(vec[:, pl.ds(0, KTILE)])
    own_totals = lax.fori_loop(
        1, samples // KTILE,
        lambda k, acc: acc + row_sums(vec[:, pl.ds(pl.multiple_of(k * KTILE, KTILE), KTILE)]),
        own_totals,
    )

    groups = row_count // group

    def chunk(i, carry):
        pair_copy(i).wait_recv()

        def one_group(q):
            out = None
            for kt in range(span // KTILE):
                at = [pl.ds(g * span + kt * KTILE, KTILE) for g in range(TREE)]
                pieces = {}
                for half in range(2):
                    js = range(half * cols // SUB // 2, (half + 1) * cols // SUB // 2)
                    theirs = {j: [arrived[i, pl.ds(j * SUB, SUB), o] for o in at] for j in js}
                    for r in range(group):
                        mine = [wide[q * group + r, :, o] for o in at]
                        for j in js:
                            pieces[r, j] = tree_sum(
                                [jnp.minimum(x, y) for x, y in zip(mine, theirs[j])]
                            )
                sums = row_sums(jnp.concatenate([pieces[at_] for at_ in sorted(pieces)], axis=0))
                out = sums if out is None else out + sums
            part[i, pl.ds(q, 1), :] = out[0:1, :]

        def groups_step(q, c):
            for k in range(UNROLL):
                one_group(q * UNROLL + k)
            return c

        lax.fori_loop(0, groups // UNROLL, groups_step, 0)
        part[i, pl.ds(groups, 8), :] = own_totals
        part[i, pl.ds(groups + 1, 1), pl.ds(0, cols)] = row_sums(arrived[i])[0:1, :]

        @pl.when(i < n_samp - 1)
        def _():
            part_copy(i).start()

        return carry

    lax.fori_loop(0, n_samp, chunk, 0)

    total = part[n_samp - 1]
    for i in range(n_samp - 1):
        part_copy(i).wait_recv()
        total = total + part_in[i]
    total_ref[...] = total

    for i in range(n_samp):
        pair_copy(i).wait_send()
    for i in range(n_samp - 1):
        part_copy(i).wait_send()
    for m in range(1, n_samp):
        next_copy(m).wait()
    own_out.wait()


def fused_body(n_vblk, n_samp, vectors, partner, next_rows):
    rows, samples = vectors.shape
    cols = rows // n_samp
    groups = rows * cols // ROWS_PER_DOT
    part_rows = groups + 8
    next_count = next_rows.shape[0]
    hbm = pl.BlockSpec(memory_space=pl.ANY)
    dma = pltpu.SemaphoreType.DMA
    total, next_block = pl.pallas_call(
        functools.partial(kernel, n_vblk, n_samp),
        out_shape=(
            jax.ShapeDtypeStruct((part_rows, ROWS_PER_DOT), jnp.float32),
            jax.ShapeDtypeStruct((next_count * n_samp, samples), next_rows.dtype),
        ),
        in_specs=[hbm, hbm, hbm],
        out_specs=(pl.BlockSpec(memory_space=pltpu.VMEM), hbm),
        scratch_shapes=[
            pltpu.VMEM((rows, samples), jnp.bfloat16),
            pltpu.VMEM((rows, SUB, samples), jnp.bfloat16),
            pltpu.VMEM((n_samp, cols, samples), jnp.bfloat16),
            pltpu.VMEM((next_count, samples), jnp.bfloat16),
            pltpu.VMEM((n_samp, part_rows, ROWS_PER_DOT), jnp.float32),
            pltpu.VMEM((n_samp - 1, part_rows, ROWS_PER_DOT), jnp.float32),
            dma, dma((2,)),
            dma((n_samp,)), dma((n_samp,)),
            dma((n_samp,)), dma((n_samp,)),
            dma((n_samp,)), dma((n_samp,)),
        ],
        compiler_params=pltpu.CompilerParams(
            collective_id=0, has_side_effects=True, vmem_limit_bytes=VMEM_BYTES
        ),
        name="similarity",
    )(vectors, partner, next_rows)
    numerators = total[:groups].reshape(rows, cols)
    own_totals = total[groups, :rows][:, None]
    pair_totals = total[groups + 1, :cols][None, :]
    return (2.0 * numerators / (own_totals + pair_totals), next_block)


def body(n_vblk, n_samp, vectors, partner, next_rows):
    rows, samples = vectors.shape
    cols = rows // n_samp
    fits = (
        n_vblk > 2
        and n_samp > 1
        and n_samp & (n_samp - 1) == 0
        and rows == ROWS_PER_DOT
        and cols % ALIGN == 0
        and samples % (TREE * KTILE) == 0
        and next_rows.shape[0] % ALIGN == 0
        and rows * SUB * samples * 2 + 4 * rows * samples * 2 <= VMEM_BYTES
    )
    if fits:
        return fused_body(n_vblk, n_samp, vectors, partner, next_rows)
    return plain_body(vectors, partner, next_rows)


def solution(mesh):
    in_specs = (P("vblk", "samp"), P("vblk", "samp"), P(("vblk", "samp"), None))
    out_specs = (P("vblk", "samp"), P("vblk", "samp"))
    step = functools.partial(body, mesh.shape["vblk"], mesh.shape["samp"])
    return jax.shard_map(step, mesh=mesh, in_specs=in_specs, out_specs=out_specs, check_vma=False)
```

```python
import functools

import jax
import jax.numpy as jnp
from jax import lax
from jax.experimental import pallas as pl
from jax.experimental.pallas import tpu as pltpu
from jax.sharding import PartitionSpec as P

MESH = pl.DeviceIdType.MESH
SUB = 8
ALIGN = 16
WIDTH = 256
UNROLL = 2
TREE = 8
KTILE = 256
ROWS_PER_DOT = 256
VMEM_BYTES = 60 * 1024 * 1024


def from_behind(value, axis, steps):
    count = lax.axis_size(axis)
    pairs = [(source, (source + steps) % count) for source in range(count)]
    return lax.ppermute(value, axis, pairs)


def pair_terms(row_block, col_block):
    row_count = row_block.shape[0]
    grouped = row_block.reshape(row_count // 8, 8, row_block.shape[1])

    def group_sums(row_group):
        return jnp.sum(
            jnp.minimum(row_group[:, None, :], col_block[None, :, :]), axis=2, dtype=jnp.float32
        )

    numerators = lax.map(group_sums, grouped).reshape(row_count, col_block.shape[0])
    row_totals = jnp.sum(row_block, axis=1, dtype=jnp.float32)[:, None]
    col_totals = jnp.sum(col_block, axis=1, dtype=jnp.float32)[None, :]
    return (numerators, row_totals, col_totals)


def plain_body(vectors, partner, next_rows):
    next_block = lax.all_to_all(next_rows, "samp", split_axis=1, concat_axis=0, tiled=True)
    arrived = from_behind(partner, "vblk", 1)
    numerators, row_totals, col_totals = pair_terms(vectors, arrived)
    numerators, col_totals = (
        lax.psum_scatter(numerators, "samp", scatter_dimension=1, tiled=True),
        lax.psum_scatter(col_totals, "samp", scatter_dimension=1, tiled=True),
    )
    row_totals = lax.psum(row_totals, "samp")
    metric = 2.0 * numerators / (row_totals + col_totals)
    return (metric, next_block)


def flipped(index, mask, count):
    out = 0
    bit = 1
    while bit < count:
        out = out + lax.rem(lax.div(index, bit) + lax.div(mask, bit), 2) * bit
        bit *= 2
    return out


def tree_sum(values):
    while len(values) > 1:
        values = [values[i] + values[i + 1] for i in range(0, len(values), 2)]
    return values[0]


def row_sums(block):
    ones = jnp.ones((8, block.shape[1]), jnp.bfloat16)
    return lax.dot_general(
        ones, block, (((1,), (1,)), ((), ())), preferred_element_type=jnp.float32
    )


def kernel(
    n_vblk, n_samp,
    vec_hbm, partner_hbm, next_hbm,
    total_ref, block_hbm,
    vec, wide, arrived, own_piece, part, part_in,
    vec_sem, piece_sem, pair_send, pair_recv, next_send, next_recv, part_send, part_recv,
):
    b = lax.axis_index("vblk")
    s = lax.axis_index("samp")
    up = lax.rem(b + 1, n_vblk)
    down = lax.rem(b + n_vblk - 1, n_vblk)
    row_count, samples = vec.shape
    cols = row_count // n_samp
    next_count = next_hbm.shape[0]
    group = ROWS_PER_DOT // cols
    span = samples // TREE

    vec_copy = pltpu.make_async_copy(vec_hbm, vec, vec_sem)
    vec_copy.start()
    own_in = pltpu.make_async_copy(
        next_hbm.at[:, pl.ds(pl.multiple_of(s * samples, samples), samples)],
        own_piece, piece_sem.at[0],
    )
    own_in.start()

    barrier = pltpu.get_barrier_semaphore()
    for neighbour in (up, down):
        pl.semaphore_signal(barrier, inc=1, device_id=(neighbour, s), device_id_type=MESH)
    for m in range(1, n_samp):
        pl.semaphore_signal(
            barrier, inc=1, device_id=(b, flipped(s, m, n_samp)), device_id_type=MESH
        )
    pl.semaphore_wait(barrier, n_samp + 1)

    def pair_copy(i):
        owner = flipped(s, n_samp - 1 - i, n_samp)
        return pltpu.make_async_remote_copy(
            src_ref=partner_hbm.at[pl.ds(pl.multiple_of(owner * cols, cols), cols), :],
            dst_ref=arrived.at[i],
            send_sem=pair_send.at[i], recv_sem=pair_recv.at[i],
            device_id=(up, s), device_id_type=MESH,
        )

    def next_copy(m):
        peer = flipped(s, m, n_samp)
        return pltpu.make_async_remote_copy(
            src_ref=next_hbm.at[:, pl.ds(pl.multiple_of(peer * samples, samples), samples)],
            dst_ref=block_hbm.at[pl.ds(pl.multiple_of(s * next_count, next_count), next_count), :],
            send_sem=next_send.at[m], recv_sem=next_recv.at[m],
            device_id=(b, peer), device_id_type=MESH,
        )

    def part_copy(i):
        peer = flipped(s, n_samp - 1 - i, n_samp)
        return pltpu.make_async_remote_copy(
            src_ref=part.at[i], dst_ref=part_in.at[i],
            send_sem=part_send.at[i], recv_sem=part_recv.at[i],
            device_id=(b, peer), device_id_type=MESH,
        )

    for i in range(n_samp):
        pair_copy(i).start()
    for m in range(1, n_samp):
        next_copy(m).start()

    own_in.wait()
    own_out = pltpu.make_async_copy(
        own_piece,
        block_hbm.at[pl.ds(pl.multiple_of(s * next_count, next_count), next_count), :],
        piece_sem.at[1],
    )
    own_out.start()

    vec_copy.wait()

    def widen(t, carry):
        first = pl.multiple_of(t * ALIGN, ALIGN)
        for c in range(samples // WIDTH):
            lanes = pl.ds(c * WIDTH, WIDTH)
            rows = vec[pl.ds(first, ALIGN), lanes].astype(jnp.float32)
            for r in range(ALIGN):
                wide[first + r, :, lanes] = jnp.broadcast_to(
                    rows[r:r + 1, :], (SUB, WIDTH)
                ).astype(jnp.bfloat16)
        return carry

    lax.fori_loop(0, row_count // ALIGN, widen, 0)

    own_totals = row_sums(vec[:, pl.ds(0, KTILE)])
    own_totals = lax.fori_loop(
        1, samples // KTILE,
        lambda k, acc: acc + row_sums(vec[:, pl.ds(pl.multiple_of(k * KTILE, KTILE), KTILE)]),
        own_totals,
    )

    groups = row_count // group

    def chunk(i, carry):
        pair_copy(i).wait_recv()

        def one_group(q):
            out = None
            for kt in range(span // KTILE):
                at = [pl.ds((kt * TREE + g) * KTILE, KTILE) for g in range(TREE)]
                pieces = {}
                for half in range(2):
                    js = range(half * cols // SUB // 2, (half + 1) * cols // SUB // 2)
                    theirs = {j: [arrived[i, pl.ds(j * SUB, SUB), o] for o in at] for j in js}
                    for r in range(group):
                        mine = [wide[r * groups + q, :, o] for o in at]
                        for j in js:
                            pieces[r, j] = tree_sum(
                                [jnp.minimum(x, y) for x, y in zip(mine, theirs[j])]
                            )
                minima = jnp.stack([pieces[key] for key in sorted(pieces)])
                sums = row_sums(minima.reshape(ROWS_PER_DOT, KTILE))
                out = sums if out is None else out + sums
            part[i, pl.ds(q, 1), :] = out[0:1, :]

        def groups_step(q, c):
            for k in range(UNROLL):
                one_group(q * UNROLL + k)
            return c

        lax.fori_loop(0, groups // UNROLL, groups_step, 0)
        part[i, pl.ds(groups, 8), :] = own_totals
        part[i, pl.ds(groups + 1, 1), pl.ds(0, cols)] = row_sums(arrived[i])[0:1, :]

        @pl.when(i < n_samp - 1)
        def _():
            part_copy(i).start()

        return carry

    lax.fori_loop(0, n_samp, chunk, 0)

    total = part[n_samp - 1]
    for i in range(n_samp - 1):
        part_copy(i).wait_recv()
        total = total + part_in[i]
    total_ref[...] = total

    for i in range(n_samp):
        pair_copy(i).wait_send()
    for i in range(n_samp - 1):
        part_copy(i).wait_send()
    for m in range(1, n_samp):
        next_copy(m).wait()
    own_out.wait()


def finish(groups, cols, total_ref, block_in, metric_ref, block_out, pieces, in_sems, out_sems):
    count, rows, _ = pieces.shape

    def take(i):
        return pltpu.make_async_copy(
            block_in.at[pl.ds(i * rows, rows), :], pieces.at[i], in_sems.at[i]
        )

    def give(i):
        return pltpu.make_async_copy(
            pieces.at[i], block_out.at[pl.ds(i * rows, rows), :], out_sems.at[i]
        )

    for i in range(count):
        take(i).start()
    turned = total_ref[pl.ds(0, groups), :].T
    numerators = jnp.concatenate(
        [turned[first:first + cols, :] for first in range(0, turned.shape[0], cols)], axis=1
    )
    own_totals = total_ref[pl.ds(groups, 1), :]
    pair_totals = total_ref[pl.ds(groups, 8), :].T[:cols, 1:2]
    metric_ref[...] = 2.0 * numerators / (own_totals + pair_totals)
    for i in range(count):
        take(i).wait()
        give(i).start()
    for i in range(count):
        give(i).wait()


def fused_body(n_vblk, n_samp, vectors, partner, next_rows):
    rows, samples = vectors.shape
    cols = rows // n_samp
    groups = rows * cols // ROWS_PER_DOT
    part_rows = groups + 8
    next_count = next_rows.shape[0]
    hbm = pl.BlockSpec(memory_space=pl.ANY)
    dma = pltpu.SemaphoreType.DMA
    total, next_block = pl.pallas_call(
        functools.partial(kernel, n_vblk, n_samp),
        out_shape=(
            jax.ShapeDtypeStruct((part_rows, ROWS_PER_DOT), jnp.float32),
            jax.ShapeDtypeStruct((next_count * n_samp, samples), next_rows.dtype),
        ),
        in_specs=[hbm, hbm, hbm],
        out_specs=(pl.BlockSpec(memory_space=pltpu.VMEM), hbm),
        scratch_shapes=[
            pltpu.VMEM((rows, samples), jnp.bfloat16),
            pltpu.VMEM((rows, SUB, samples), jnp.bfloat16),
            pltpu.VMEM((n_samp, cols, samples), jnp.bfloat16),
            pltpu.VMEM((next_count, samples), jnp.bfloat16),
            pltpu.VMEM((n_samp, part_rows, ROWS_PER_DOT), jnp.float32),
            pltpu.VMEM((n_samp - 1, part_rows, ROWS_PER_DOT), jnp.float32),
            dma, dma((2,)),
            dma((n_samp,)), dma((n_samp,)),
            dma((n_samp,)), dma((n_samp,)),
            dma((n_samp,)), dma((n_samp,)),
        ],
        compiler_params=pltpu.CompilerParams(
            collective_id=0, has_side_effects=True, vmem_limit_bytes=VMEM_BYTES
        ),
        name="similarity",
    )(vectors, partner, next_rows)
    metric, next_block = pl.pallas_call(
        functools.partial(finish, groups, cols),
        out_shape=(
            jax.ShapeDtypeStruct((cols, rows), jnp.float32),
            jax.ShapeDtypeStruct(next_block.shape, next_block.dtype),
        ),
        in_specs=[pl.BlockSpec(memory_space=pltpu.VMEM), hbm],
        out_specs=(pl.BlockSpec(memory_space=pltpu.VMEM), hbm),
        scratch_shapes=[
            pltpu.VMEM((n_samp, next_count, samples), next_rows.dtype),
            dma((n_samp,)), dma((n_samp,)),
        ],
        name="finish",
    )(total, next_block)
    return (metric.T, next_block)


def body(n_vblk, n_samp, vectors, partner, next_rows):
    rows, samples = vectors.shape
    cols = rows // n_samp
    fits = (
        n_vblk > 2
        and n_samp > 1
        and n_samp & (n_samp - 1) == 0
        and rows == ROWS_PER_DOT
        and cols % ALIGN == 0
        and samples % (TREE * KTILE) == 0
        and next_rows.shape[0] % ALIGN == 0
        and rows * SUB * samples * 2 + 4 * rows * samples * 2 <= VMEM_BYTES
        and next_rows.shape[0] * n_samp == rows
    )
    if fits:
        return fused_body(n_vblk, n_samp, vectors, partner, next_rows)
    return plain_body(vectors, partner, next_rows)


def solution(mesh):
    in_specs = (P("vblk", "samp"), P("vblk", "samp"), P(("vblk", "samp"), None))
    out_specs = (P("vblk", "samp"), P("vblk", "samp"))
    step = functools.partial(body, mesh.shape["vblk"], mesh.shape["samp"])
    return jax.shard_map(step, mesh=mesh, in_specs=in_specs, out_specs=out_specs, check_vma=False)
```

```python
import functools

import jax
import jax.numpy as jnp
from jax import lax
from jax.experimental import pallas as pl
from jax.experimental.pallas import tpu as pltpu
from jax.sharding import PartitionSpec as P

MESH = pl.DeviceIdType.MESH
SUB = 8
ALIGN = 16
WIDTH = 256
UNROLL = 8
TREE = 8
KTILE = 256
ROWS_PER_DOT = 256
VMEM_BYTES = 60 * 1024 * 1024


def from_behind(value, axis, steps):
    count = lax.axis_size(axis)
    pairs = [(source, (source + steps) % count) for source in range(count)]
    return lax.ppermute(value, axis, pairs)


def pair_terms(row_block, col_block):
    row_count = row_block.shape[0]
    grouped = row_block.reshape(row_count // 8, 8, row_block.shape[1])

    def group_sums(row_group):
        return jnp.sum(
            jnp.minimum(row_group[:, None, :], col_block[None, :, :]), axis=2, dtype=jnp.float32
        )

    numerators = lax.map(group_sums, grouped).reshape(row_count, col_block.shape[0])
    row_totals = jnp.sum(row_block, axis=1, dtype=jnp.float32)[:, None]
    col_totals = jnp.sum(col_block, axis=1, dtype=jnp.float32)[None, :]
    return (numerators, row_totals, col_totals)


def plain_body(vectors, partner, next_rows):
    next_block = lax.all_to_all(next_rows, "samp", split_axis=1, concat_axis=0, tiled=True)
    arrived = from_behind(partner, "vblk", 1)
    numerators, row_totals, col_totals = pair_terms(vectors, arrived)
    numerators, col_totals = (
        lax.psum_scatter(numerators, "samp", scatter_dimension=1, tiled=True),
        lax.psum_scatter(col_totals, "samp", scatter_dimension=1, tiled=True),
    )
    row_totals = lax.psum(row_totals, "samp")
    metric = 2.0 * numerators / (row_totals + col_totals)
    return (metric, next_block)


def flipped(index, mask, count):
    out = 0
    bit = 1
    while bit < count:
        out = out + lax.rem(lax.div(index, bit) + lax.div(mask, bit), 2) * bit
        bit *= 2
    return out


def tree_sum(values):
    while len(values) > 1:
        values = [values[i] + values[i + 1] for i in range(0, len(values), 2)]
    return values[0]


def row_sums(block):
    ones = jnp.ones((8, block.shape[1]), jnp.bfloat16)
    return lax.dot_general(
        ones, block, (((1,), (1,)), ((), ())), preferred_element_type=jnp.float32
    )


def kernel(
    n_vblk, n_samp,
    vec_hbm, partner_hbm, next_hbm,
    total_ref, block_hbm,
    vec, wide, arrived, own_piece, part, part_in,
    vec_sem, piece_sem, pair_send, pair_recv, next_send, next_recv, part_send, part_recv,
):
    b = lax.axis_index("vblk")
    s = lax.axis_index("samp")
    up = lax.rem(b + 1, n_vblk)
    down = lax.rem(b + n_vblk - 1, n_vblk)
    row_count, samples = vec.shape
    cols = row_count // n_samp
    next_count = next_hbm.shape[0]
    group = ROWS_PER_DOT // cols
    span = samples // TREE

    vec_copy = pltpu.make_async_copy(vec_hbm, vec, vec_sem)
    vec_copy.start()
    own_in = pltpu.make_async_copy(
        next_hbm.at[:, pl.ds(pl.multiple_of(s * samples, samples), samples)],
        own_piece, piece_sem.at[0],
    )
    own_in.start()

    barrier = pltpu.get_barrier_semaphore()
    for neighbour in (up, down):
        pl.semaphore_signal(barrier, inc=1, device_id=(neighbour, s), device_id_type=MESH)
    for m in range(1, n_samp):
        pl.semaphore_signal(
            barrier, inc=1, device_id=(b, flipped(s, m, n_samp)), device_id_type=MESH
        )
    pl.semaphore_wait(barrier, n_samp + 1)

    def pair_copy(i):
        owner = flipped(s, n_samp - 1 - i, n_samp)
        return pltpu.make_async_remote_copy(
            src_ref=partner_hbm.at[pl.ds(pl.multiple_of(owner * cols, cols), cols), :],
            dst_ref=arrived.at[i],
            send_sem=pair_send.at[i], recv_sem=pair_recv.at[i],
            device_id=(up, s), device_id_type=MESH,
        )

    def next_copy(m):
        peer = flipped(s, m, n_samp)
        return pltpu.make_async_remote_copy(
            src_ref=next_hbm.at[:, pl.ds(pl.multiple_of(peer * samples, samples), samples)],
            dst_ref=block_hbm.at[pl.ds(pl.multiple_of(s * next_count, next_count), next_count), :],
            send_sem=next_send.at[m], recv_sem=next_recv.at[m],
            device_id=(b, peer), device_id_type=MESH,
        )

    def part_copy(i):
        peer = flipped(s, n_samp - 1 - i, n_samp)
        return pltpu.make_async_remote_copy(
            src_ref=part.at[i], dst_ref=part_in.at[i],
            send_sem=part_send.at[i], recv_sem=part_recv.at[i],
            device_id=(b, peer), device_id_type=MESH,
        )

    for i in range(n_samp):
        pair_copy(i).start()
    for m in range(1, n_samp):
        next_copy(m).start()

    own_in.wait()
    own_out = pltpu.make_async_copy(
        own_piece,
        block_hbm.at[pl.ds(pl.multiple_of(s * next_count, next_count), next_count), :],
        piece_sem.at[1],
    )
    own_out.start()

    vec_copy.wait()

    def widen(t, carry):
        first = pl.multiple_of(t * ALIGN, ALIGN)
        for c in range(samples // WIDTH):
            lanes = pl.ds(c * WIDTH, WIDTH)
            rows = vec[pl.ds(first, ALIGN), lanes].astype(jnp.float32)
            for r in range(ALIGN):
                wide[first + r, :, lanes] = jnp.broadcast_to(
                    rows[r:r + 1, :], (SUB, WIDTH)
                ).astype(jnp.bfloat16)
        return carry

    lax.fori_loop(0, row_count // ALIGN, widen, 0)

    own_totals = row_sums(vec[:, pl.ds(0, KTILE)])
    own_totals = lax.fori_loop(
        1, samples // KTILE,
        lambda k, acc: acc + row_sums(vec[:, pl.ds(pl.multiple_of(k * KTILE, KTILE), KTILE)]),
        own_totals,
    )

    groups = row_count // group

    def chunk(i, carry):
        pair_copy(i).wait_recv()

        def one_group(q):
            out = None
            for kt in range(span // KTILE):
                at = [pl.ds((kt * TREE + g) * KTILE, KTILE) for g in range(TREE)]
                pieces = {}
                for half in range(2):
                    js = range(half * cols // SUB // 2, (half + 1) * cols // SUB // 2)
                    theirs = {j: [arrived[i, pl.ds(j * SUB, SUB), o] for o in at] for j in js}
                    for r in range(group):
                        mine = [wide[r * groups + q, :, o] for o in at]
                        for j in js:
                            pieces[r, j] = tree_sum(
                                [jnp.minimum(x, y) for x, y in zip(mine, theirs[j])]
                            )
                minima = jnp.stack([pieces[key] for key in sorted(pieces)])
                sums = row_sums(minima.reshape(ROWS_PER_DOT, KTILE))
                out = sums if out is None else out + sums
            part[i, pl.ds(q, 1), :] = out[0:1, :]

        def groups_step(q, c):
            for k in range(UNROLL):
                one_group(q * UNROLL + k)
            return c

        lax.fori_loop(0, groups // UNROLL, groups_step, 0)
        part[i, pl.ds(groups, 8), :] = own_totals
        part[i, pl.ds(groups + 1, 1), pl.ds(0, cols)] = row_sums(arrived[i])[0:1, :]

        @pl.when(i < n_samp - 1)
        def _():
            part_copy(i).start()

        return carry

    lax.fori_loop(0, n_samp, chunk, 0)

    total = part[n_samp - 1]
    for i in range(n_samp - 1):
        part_copy(i).wait_recv()
        total = total + part_in[i]
    total_ref[...] = total

    for i in range(n_samp):
        pair_copy(i).wait_send()
    for i in range(n_samp - 1):
        part_copy(i).wait_send()
    for m in range(1, n_samp):
        next_copy(m).wait()
    own_out.wait()


def finish(
    groups, cols, total_hbm, block_in, metric_hbm, block_out,
    total_ref, metric_ref, pieces, in_sems, out_sems, end_sems,
):
    count, rows, _ = pieces.shape

    def take(i):
        return pltpu.make_async_copy(
            block_in.at[pl.ds(i * rows, rows), :], pieces.at[i], in_sems.at[i]
        )

    def give(i):
        return pltpu.make_async_copy(
            pieces.at[i], block_out.at[pl.ds(i * rows, rows), :], out_sems.at[i]
        )

    total_in = pltpu.make_async_copy(total_hbm, total_ref, end_sems.at[0])
    metric_out = pltpu.make_async_copy(metric_ref, metric_hbm, end_sems.at[1])
    total_in.start()
    for i in range(count):
        take(i).start()
    total_in.wait()
    turned = total_ref[pl.ds(0, groups), :].T
    numerators = jnp.concatenate(
        [turned[first:first + cols, :] for first in range(0, turned.shape[0], cols)], axis=1
    )
    own_totals = total_ref[pl.ds(groups, 1), :]
    pair_totals = total_ref[pl.ds(groups, 8), :].T[:cols, 1:2]
    metric_ref[...] = 2.0 * numerators / (own_totals + pair_totals)
    metric_out.start()
    for i in range(count):
        take(i).wait()
        give(i).start()
    for i in range(count):
        give(i).wait()
    metric_out.wait()


def fused_body(n_vblk, n_samp, vectors, partner, next_rows):
    rows, samples = vectors.shape
    cols = rows // n_samp
    groups = rows * cols // ROWS_PER_DOT
    part_rows = groups + 8
    next_count = next_rows.shape[0]
    hbm = pl.BlockSpec(memory_space=pl.ANY)
    dma = pltpu.SemaphoreType.DMA
    total, next_block = pl.pallas_call(
        functools.partial(kernel, n_vblk, n_samp),
        out_shape=(
            jax.ShapeDtypeStruct((part_rows, ROWS_PER_DOT), jnp.float32),
            jax.ShapeDtypeStruct((next_count * n_samp, samples), next_rows.dtype),
        ),
        in_specs=[hbm, hbm, hbm],
        out_specs=(pl.BlockSpec(memory_space=pltpu.VMEM), hbm),
        scratch_shapes=[
            pltpu.VMEM((rows, samples), jnp.bfloat16),
            pltpu.VMEM((rows, SUB, samples), jnp.bfloat16),
            pltpu.VMEM((n_samp, cols, samples), jnp.bfloat16),
            pltpu.VMEM((next_count, samples), jnp.bfloat16),
            pltpu.VMEM((n_samp, part_rows, ROWS_PER_DOT), jnp.float32),
            pltpu.VMEM((n_samp - 1, part_rows, ROWS_PER_DOT), jnp.float32),
            dma, dma((2,)),
            dma((n_samp,)), dma((n_samp,)),
            dma((n_samp,)), dma((n_samp,)),
            dma((n_samp,)), dma((n_samp,)),
        ],
        compiler_params=pltpu.CompilerParams(
            collective_id=0, has_side_effects=True, vmem_limit_bytes=VMEM_BYTES
        ),
        name="similarity",
    )(vectors, partner, next_rows)
    metric, next_block = pl.pallas_call(
        functools.partial(finish, groups, cols),
        out_shape=(
            jax.ShapeDtypeStruct((cols, rows), jnp.float32),
            jax.ShapeDtypeStruct(next_block.shape, next_block.dtype),
        ),
        in_specs=[hbm, hbm],
        out_specs=(hbm, hbm),
        scratch_shapes=[
            pltpu.VMEM((part_rows, ROWS_PER_DOT), jnp.float32),
            pltpu.VMEM((cols, rows), jnp.float32),
            pltpu.VMEM((n_samp, next_count, samples), next_rows.dtype),
            dma((n_samp,)), dma((n_samp,)), dma((2,)),
        ],
        name="finish",
    )(total, next_block)
    return (metric.T, next_block)


def body(n_vblk, n_samp, vectors, partner, next_rows):
    rows, samples = vectors.shape
    cols = rows // n_samp
    fits = (
        n_vblk > 2
        and n_samp > 1
        and n_samp & (n_samp - 1) == 0
        and rows == ROWS_PER_DOT
        and cols % ALIGN == 0
        and cols % UNROLL == 0
        and samples % (TREE * KTILE) == 0
        and next_rows.shape[0] % ALIGN == 0
        and rows * SUB * samples * 2 + 4 * rows * samples * 2 <= VMEM_BYTES
        and next_rows.shape[0] * n_samp == rows
    )
    if fits:
        return fused_body(n_vblk, n_samp, vectors, partner, next_rows)
    return plain_body(vectors, partner, next_rows)


def solution(mesh):
    in_specs = (P("vblk", "samp"), P("vblk", "samp"), P(("vblk", "samp"), None))
    out_specs = (P("vblk", "samp"), P("vblk", "samp"))
    step = functools.partial(body, mesh.shape["vblk"], mesh.shape["samp"])
    return jax.shard_map(step, mesh=mesh, in_specs=in_specs, out_specs=out_specs, check_vma=False)
```
